32 devices in a mesh: tp: 4 (over y, x), dp: 8 (over z, core).
Axes of the slice: x: 2, y: 2, z: 4, core: 2. Of those that a mesh axis runs over, the one named last changes fastest.
Arguments:
- activations: bfloat16 [2, 8192, 8192], P(None, 'dp', 'tp'), may hold values from -72 to 72
- out_grads: bfloat16 [2, 8192, 2048], P(None, 'dp'), may hold values from -2 to 2
- master: float32 [8192, 2, 2048], P(('tp', 'dp')), may hold values from -1.2 to 1.2
- first_moment: float32 [8192, 2, 2048], P(('tp', 'dp')), may hold values from -1.8 to 1.8
- second_moment: float32 [8192, 2, 2048], P(('tp', 'dp')), may hold values from 0.01 to 1
Outputs:
- new_master: float32 [8192, 2, 2048], P(('tp', 'dp'))
- new_first: float32 [8192, 2, 2048], P(('tp', 'dp'))
- new_second: float32 [8192, 2, 2048], P(('tp', 'dp'))
- weights: bfloat16 [8192, 2, 2048], P('tp')
The draws below stay inside these ranges and needn't reach their ends.
All inputs are finite; a program needn't handle non-finite values.
Results may differ from the reference program's by a relative error of at most 0.0004.
Values may be sent and summed in bfloat16 or wider, within the bound.
No kernel may reach another device: no remote copies, remote signals or barrier semaphores. Data moves between devices by JAX's collectives and lax.ppermute only.
A program may use at most 192 MiB of HBM per device.

```python
import math
import jax
import jax.numpy as jnp

D = 8192
KVW = 2048
LAYERS = 2
TOKENS = 8192


def shared_signs(key):
    sign_bits = jax.random.randint(jax.random.fold_in(key, 101), (LAYERS, TOKENS), 0, 2)
    return (2 * sign_bits - 1).astype(jnp.float32)


def draw_activations(key, part):
    token_signs = shared_signs(key)
    noise_key = jax.random.fold_in(key, 202)
    along_key = jax.random.fold_in(key, 203)
    noise = jnp.clip(jax.random.normal(noise_key, (LAYERS, TOKENS, D), jnp.float32), -6.0, 6.0)
    direction = jnp.clip(jax.random.normal(along_key, (LAYERS, D), jnp.float32), -3.0, 3.0)
    strength = 8.0
    values = 8.0 * noise + strength * token_signs[:, :, None] * direction[:, None, :]
    return values.astype(jnp.bfloat16)


def draw_out_grads(key, part):
    token_signs = shared_signs(key)
    noise_key = jax.random.fold_in(key, 302)
    along_key = jax.random.fold_in(key, 303)
    noise = jnp.clip(jax.random.normal(noise_key, (LAYERS, TOKENS, KVW), jnp.float32), -6.0, 6.0)
    direction = jnp.clip(jax.random.normal(along_key, (LAYERS, KVW), jnp.float32), -3.0, 3.0)
    values = noise * TOKENS ** (-0.5) + token_signs[:, :, None] * direction[:, None, :] * (1.0 / TOKENS)
    return values.astype(jnp.bfloat16)


def block_scale(own_key, shape, split, smallest, high):
    factor_of = 1.0
    for dim, blocks in split:
        steps = jax.random.uniform(jax.random.fold_in(jax.random.fold_in(own_key, 6), dim), (blocks,), jnp.float32, smallest / len(split), high / len(split))
        factor_of = factor_of * jnp.repeat(jnp.exp(steps), shape[dim] // blocks).reshape((-1,) + (1,) * (len(shape) - 1 - dim))
    return factor_of


def centred(key, dims, width, reach, pieces=(), dtype=jnp.bfloat16):
    values = width * jax.random.normal(key, dims, jnp.float32)
    if pieces:
        values = values * block_scale(key, dims, pieces, -0.22, 0.18)
    return jnp.clip(values, -reach, reach).astype(dtype)


def setup_inputs(seed: int = 0) -> dict:
    keys = jax.random.split(jax.random.key(seed), 6)
    return {
        "activations": draw_activations(jax.random.fold_in(keys[5], 71), 0),
        "out_grads": draw_out_grads(jax.random.fold_in(keys[5], 71), 0),
        "master": centred(keys[2], (D, LAYERS, KVW), 0.2, 1.2, ((0, 32),), jnp.float32),
        "first_moment": centred(keys[3], (D, LAYERS, KVW), 0.3, 1.8, ((0, 32),), jnp.float32),
        "second_moment": jnp.clip(jnp.exp(math.log(1.0) - 4.6051702 * jax.random.uniform(keys[4], (D, LAYERS, KVW), jnp.float32) ** block_scale(keys[4], (D, LAYERS, KVW), ((0, 32),), -0.2, 0.2)), 0.01, 1.0),
    }


beta_first = 0.9
beta_second = 0.95
first_fix = 1.0 - 0.9 ** 10
second_fix = 1.0 - 0.95 ** 10
learn_rate = 0.01
decay_rate = 0.1
epsilon = 1e-08
limit_scale = 2.0

def reference(activations, out_grads, master, first_moment, second_moment):
    grad = jnp.einsum('ltd,ltc->dlc', activations.astype(jnp.float32), out_grads.astype(jnp.float32))
    squares = jnp.sum(grad * grad)
    limit = limit_scale * math.sqrt(D * LAYERS * KVW)
    clip_factor = limit / jnp.maximum(jnp.sqrt(squares), limit)
    clipped = clip_factor * grad
    new_first = beta_first * first_moment + (1.0 - beta_first) * clipped
    new_second = beta_second * second_moment + (1.0 - beta_second) * clipped * clipped
    step_dir = new_first / first_fix / (jnp.sqrt(new_second / second_fix) + epsilon)
    new_master = master - learn_rate * (step_dir + decay_rate * master)
    return (new_master, new_first, new_second, new_master.astype(jnp.bfloat16))
```

```python
import math

import jax
import jax.numpy as jnp
from jax import lax
from jax.sharding import PartitionSpec as P

beta_first = 0.9
beta_second = 0.95
first_fix = 1.0 - 0.9**10
second_fix = 1.0 - 0.95**10
learn_rate = 0.01
decay_rate = 0.1
epsilon = 1e-08
limit_scale = 2.0
largest_product = 72.0 * 2.0
wire = jnp.float16


def adam_update(grad_own, master, first_moment, second_moment, clip_factor):
    clipped = clip_factor * grad_own
    new_first = beta_first * first_moment + (1.0 - beta_first) * clipped
    new_second = beta_second * second_moment + (1.0 - beta_second) * clipped * clipped
    step_dir = new_first / first_fix / (jnp.sqrt(new_second / second_fix) + epsilon)
    new_master = master - learn_rate * (step_dir + decay_rate * master)
    return (new_master, new_first, new_second)


def sum_everywhere(value, axes):
    for axis in axes:
        size = lax.axis_size(axis)
        if size & (size - 1):
            value = lax.psum(value, axis)
            continue
        step = 1
        while step < size:
            pairs = [(i, i ^ step) for i in range(size)]
            value = value + lax.ppermute(value, axis, pairs)
            step *= 2
    return value


def reduce_own_rows(acts, grads, own_rows):
    layers, tokens, _ = acts.shape
    size = lax.axis_size("dp")
    chips = size // 2
    index = lax.axis_index("dp")
    chip, core = index // 2, index % 2
    bound = largest_product * tokens * size
    scale = 2.0 ** -max(0, math.ceil(math.log2(bound / 65504.0)))
    partner = [(i, i ^ 1) for i in range(size)]

    def partial(d, c, l):
        start = (d * 2 + c) * own_rows
        rows = lax.dynamic_slice(acts[l], (0, start), (tokens, own_rows))
        return lax.dot_general(
            rows, grads[l], (((0,), (0,)), ((), ())), preferred_element_type=jnp.float32
        )

    def chip_sum(d, l):
        theirs = lax.ppermute(partial(d, 1 - core, l), "dp", partner)
        return partial(d, core, l) + theirs

    def widen(x):
        return 0.0 if x is None else x.astype(jnp.float32) * (1.0 / scale)

    def narrow(x):
        return (x * scale).astype(wire)

    from_left = [None] * layers
    from_right = [None] * layers
    for s in range(1, chips):
        reach = chips - s
        up = [(2 * z + c, 2 * z + 2 + c) for z in range(s) for c in range(2)]
        down = [(2 * z + c, 2 * z - 2 + c) for z in range(reach, chips) for c in range(2)]
        for l in range(layers):
            if 2 * s <= chips:
                d = jnp.where(chip < s, chip + reach, (chip + s) % chips)
                value = narrow(chip_sum(d, l) + widen(from_left[l]) + widen(from_right[l]))
                right_going = left_going = value
            else:
                right_going = narrow(chip_sum((chip + reach) % chips, l) + widen(from_left[l]))
                left_going = narrow(chip_sum((chip + s) % chips, l) + widen(from_right[l]))
            from_left[l] = lax.ppermute(right_going, "dp", up)
            from_right[l] = lax.ppermute(left_going, "dp", down)
    return [
        chip_sum(chip, l) + widen(from_left[l]) + widen(from_right[l]) for l in range(layers)
    ]


def on_device(activations, out_grads, master, first_moment, second_moment):
    own_rows = master.shape[0]
    per_layer = reduce_own_rows(activations, out_grads, own_rows)
    squares = sum(jnp.sum(g * g) for g in per_layer)
    sum_squares = sum_everywhere(squares.reshape(1, 1), ("dp", "tp"))[0, 0]
    grad_own = jnp.stack(per_layer, axis=1)
    entries = (
        own_rows * lax.axis_size("tp") * lax.axis_size("dp") * master.shape[1] * master.shape[2]
    )
    limit = limit_scale * math.sqrt(entries)
    clip_factor = limit / jnp.maximum(jnp.sqrt(sum_squares), limit)
    new_master, new_first, new_second = adam_update(
        grad_own, master, first_moment, second_moment, clip_factor
    )
    rounded = new_master.astype(jnp.bfloat16)
    tp_rows = lax.all_gather(rounded, "dp", axis=0, tiled=True)
    return (new_master, new_first, new_second, tp_rows)


def solution(mesh):
    return jax.shard_map(
        on_device,
        mesh=mesh,
        in_specs=(
            P(None, "dp", "tp"),
            P(None, "dp", None),
            P(("tp", "dp"), None, None),
            P(("tp", "dp"), None, None),
            P(("tp", "dp"), None, None),
        ),
        out_specs=(
            P(("tp", "dp"), None, None),
            P(("tp", "dp"), None, None),
            P(("tp", "dp"), None, None),
            P("tp", None, None),
        ),
        check_vma=False,
    )
```

```python
import math

import jax
import jax.numpy as jnp
from jax import lax
from jax.experimental.layout import Layout, with_layout_constraint
from jax.sharding import PartitionSpec as P

beta_first = 0.9
beta_second = 0.95
first_fix = 1.0 - 0.9**10
second_fix = 1.0 - 0.95**10
learn_rate = 0.01
decay_rate = 0.1
epsilon = 1e-08
limit_scale = 2.0
largest_product = 72.0 * 2.0
wire = jnp.float16


def adam_update(grad_own, master, first_moment, second_moment, clip_factor):
    clipped = clip_factor * grad_own
    new_first = beta_first * first_moment + (1.0 - beta_first) * clipped
    new_second = beta_second * second_moment + (1.0 - beta_second) * clipped * clipped
    step_dir = new_first / first_fix / (jnp.sqrt(new_second / second_fix) + epsilon)
    new_master = master - learn_rate * (step_dir + decay_rate * master)
    return (new_master, new_first, new_second)


def sum_everywhere(value, axes):
    for axis in axes:
        size = lax.axis_size(axis)
        if size & (size - 1):
            value = lax.psum(value, axis)
            continue
        step = 1
        while step < size:
            pairs = [(i, i ^ step) for i in range(size)]
            value = value + lax.ppermute(value, axis, pairs)
            step *= 2
    return value


def reduce_own_rows(acts, grads, own_rows):
    layers, tokens, _ = acts.shape
    size = lax.axis_size("dp")
    chips = size // 2
    index = lax.axis_index("dp")
    chip, core = index // 2, index % 2
    bound = largest_product * tokens * size
    scale = 2.0 ** -max(0, math.ceil(math.log2(bound / 65504.0)))
    partner = [(i, i ^ 1) for i in range(size)]

    def partial(d, c, l):
        start = (d * 2 + c) * own_rows
        rows = lax.dynamic_slice(acts[l], (0, start), (tokens, own_rows))
        return lax.dot_general(
            rows, grads[l], (((0,), (0,)), ((), ())), preferred_element_type=jnp.float32
        )

    def chip_sum(d, l, core):
        theirs = lax.ppermute(partial(d, 1 - core, l), "dp", partner)
        return partial(d, core, l) + theirs

    def widen(x):
        return 0.0 if x is None else x.astype(jnp.float32) * (1.0 / scale)

    def narrow(x):
        return (x * scale).astype(wire)

    from_left = [None] * layers
    from_right = [None] * layers
    for s in range(1, chips):
        reach = chips - s
        up = [(2 * z + c, 2 * z + 2 + c) for z in range(s) for c in range(2)]
        down = [(2 * z + c, 2 * z - 2 + c) for z in range(reach, chips) for c in range(2)]
        for l in range(layers):
            if 2 * s <= chips:
                d = jnp.where(chip < s, chip + reach, (chip + s) % chips)
                value = narrow(chip_sum(d, l, core) + widen(from_left[l]) + widen(from_right[l]))
                if s == 1:
                    value, core = lax.optimization_barrier((value, core))
                right_going = left_going = value
            else:
                right_going = narrow(chip_sum((chip + reach) % chips, l, core) + widen(from_left[l]))
                left_going = narrow(chip_sum((chip + s) % chips, l, core) + widen(from_right[l]))
            from_left[l] = lax.ppermute(right_going, "dp", up)
            from_right[l] = lax.ppermute(left_going, "dp", down)
    return [
        chip_sum(chip, l, core) + widen(from_left[l]) + widen(from_right[l]) for l in range(layers)
    ]


def on_device(activations, out_grads, master, first_moment, second_moment):
    own_rows = master.shape[0]
    per_layer = reduce_own_rows(activations, out_grads, own_rows)
    squares = sum(jnp.sum(g * g) for g in per_layer)
    sum_squares = sum_everywhere(squares.reshape(1, 1), ("dp", "tp"))[0, 0]
    grad_own = with_layout_constraint(jnp.stack(per_layer, axis=1), Layout((0, 1, 2)))
    entries = (
        own_rows * lax.axis_size("tp") * lax.axis_size("dp") * master.shape[1] * master.shape[2]
    )
    limit = limit_scale * math.sqrt(entries)
    clip_factor = limit / jnp.maximum(jnp.sqrt(sum_squares), limit)
    new_master, new_first, new_second = adam_update(
        grad_own, master, first_moment, second_moment, clip_factor
    )
    rounded = new_master.astype(jnp.bfloat16)
    tp_rows = lax.all_gather(rounded, "dp", axis=0, tiled=True)
    return (new_master, new_first, new_second, tp_rows)


def solution(mesh):
    return jax.shard_map(
        on_device,
        mesh=mesh,
        in_specs=(
            P(None, "dp", "tp"),
            P(None, "dp", None),
            P(("tp", "dp"), None, None),
            P(("tp", "dp"), None, None),
            P(("tp", "dp"), None, None),
        ),
        out_specs=(
            P(("tp", "dp"), None, None),
            P(("tp", "dp"), None, None),
            P(("tp", "dp"), None, None),
            P("tp", None, None),
        ),
        check_vma=False,
    )
```
